32 devices in a mesh: fsdp: 8 (over y, x, core), expert: 4 (over z).
Axes of the slice: x: 2, y: 2, z: 4, core: 2. Of those that a mesh axis runs over, the one named last changes fastest.
Arguments:
- tokens: bfloat16 [512, 4096], P('fsdp', 'expert'), may hold values from -6 to 6
- cotangent: bfloat16 [512, 4096], P('fsdp', 'expert'), may hold values from -0.29882812 to 0.29882812
- experts: int32 [512, 2], P('fsdp'), may hold values from 0 to 3, as said below
- slots: int32 [512, 2], P('fsdp'), may hold values from 0 to 39, as said below
- gates: float32 [512, 2], P('fsdp'), may hold values from 0.2 to 1
- w_gate: bfloat16 [4, 7168, 4096], P('expert', 'fsdp'), may hold values from -0.09375 to 0.09375
- w_up: bfloat16 [4, 7168, 4096], P('expert', 'fsdp'), may hold values from -0.09375 to 0.09375
- w_down: bfloat16 [4, 7168, 4096], P('expert', 'fsdp'), may hold values from -0.0625 to 0.0625
Outputs:
- grad_gate: bfloat16 [4, 7168, 4096], P('expert', 'fsdp')
- grad_up: bfloat16 [4, 7168, 4096], P('expert', 'fsdp')
- grad_down: bfloat16 [4, 7168, 4096], P('expert', 'fsdp')
The draws below stay inside these ranges and needn't reach their ends.
Inputs may be any that keep to these rules, and one draw needn't show every extreme that they name: A token's 2 experts differ. In each aligned batch of 64 tokens no expert is chosen more than 40 times and some expert exactly 40 times. Within one batch of 64 tokens, the choices of the same expert have distinct slots.
All inputs are finite; a program needn't handle non-finite values.
Results may differ from the reference program's by a relative error of at most 0.0058.
Values may be sent and summed in bfloat16 or wider, within the bound.
No kernel may reach another device: no remote copies, remote signals or barrier semaphores. Data moves between devices by JAX's collectives and lax.ppermute only.
A program may use at most 128 MiB of HBM per device.

```python
import jax
import jax.numpy as jnp
from jax import lax

D = 4096
FFW = 7168
TOPK = 2
TOK_UNIT = 16
EXPERTS = 4
TOK_F = 64
CAP = 40
TOKENS = 512


def routing_block(block_key):
    experts_count = EXPERTS
    per_batch = TOK_F
    capacity = CAP
    surplus = capacity - 2 * TOK_UNIT
    key_shift, key_label, key_slots, key_order = jax.random.split(block_key, 4)
    shifts = jax.random.randint(key_shift, (experts_count // 2,), 0, surplus + 1)
    shifts = shifts.at[0].set(surplus)
    counts = jnp.stack([2 * TOK_UNIT + shifts, 2 * TOK_UNIT - shifts], axis=1).reshape(experts_count)
    ends = jnp.cumsum(counts)
    starts = ends - counts
    positions = jnp.arange(2 * per_batch)
    labels = jnp.sum((positions[:, None] >= ends[None, :]).astype(jnp.int32), axis=1)
    ranks = positions - starts[labels]
    relabel = jax.random.permutation(key_label, experts_count)
    slot_tables = jax.vmap(lambda small_key: jax.random.permutation(small_key, capacity))(jax.random.split(key_slots, experts_count))
    chosen = relabel[labels]
    placed = slot_tables[labels, ranks]
    order = jax.random.permutation(key_order, per_batch)
    first = jnp.stack([chosen[order], placed[order]], axis=1)
    second = jnp.stack([chosen[order + per_batch], placed[order + per_batch]], axis=1)
    return jnp.stack([first, second], axis=1).astype(jnp.int32)


def routing_table(key):
    batches = TOKENS // TOK_F
    blocks = jax.vmap(routing_block)(jax.random.split(jax.random.fold_in(key, 7), batches))
    table = blocks.reshape(TOKENS, TOPK, 2)
    return (table[:, :, 0], table[:, :, 1])


def draw_experts(key, part):
    return routing_table(key)[0]


def draw_slots(key, part):
    return routing_table(key)[1]


def level_of(key, shape, shards, low, high):
    def one(dim, shards_of):
        steps = jax.random.uniform(jax.random.fold_in(jax.random.fold_in(key, 6), dim), (shards_of,), jnp.float32, low / len(shards), high / len(shards))
        return jnp.repeat(jnp.exp(steps), shape[dim] // shards_of).reshape((-1,) + (1,) * (len(shape) - dim - 1))

    factor_of = one(*shards[0])
    for cut in shards[1:]:
        factor_of = factor_of * one(*cut)
    return factor_of


def scatter_about(key, dims, scale, limit, pieces=(), dtype=jnp.bfloat16):
    entries = scale * jax.random.normal(key, dims, jnp.float32)
    if pieces:
        entries = entries * level_of(key, dims, pieces, -0.22, 0.18)
    return jnp.clip(entries, -limit, limit).astype(dtype)


def setup_inputs(seed: int = 0) -> dict:
    seeds = jax.random.split(jax.random.key(seed), 9)
    tokens = scatter_about(seeds[0], (TOKENS, D), 1.0, 6.0, ((0, 8), (1, 4)))
    cotangent = scatter_about(seeds[1], (TOKENS, D), 0.05, 0.29882812, ((0, 8), (1, 4)))
    experts = draw_experts(jax.random.fold_in(seeds[8], 71), 0)
    slots = draw_slots(jax.random.fold_in(seeds[8], 71), 0)
    gates = jnp.clip(0.2 + 0.8 * jax.random.uniform(seeds[4], (TOKENS, TOPK), jnp.float32) ** level_of(seeds[4], (TOKENS, TOPK), ((0, 8),), -0.2, 0.2), 0.2, 1.0)
    w_gate = scatter_about(seeds[5], (EXPERTS, FFW, D), D ** -0.5, 0.09375, ((0, 4), (1, 8)))
    w_up = scatter_about(seeds[6], (EXPERTS, FFW, D), D ** -0.5, 0.09375, ((0, 4), (1, 8)))
    w_down = scatter_about(seeds[7], (EXPERTS, FFW, D), FFW ** -0.5, 0.0625, ((0, 4), (1, 8)))
    return {"tokens": tokens, "cotangent": cotangent, "experts": experts, "slots": slots, "gates": gates, "w_gate": w_gate, "w_up": w_up, "w_down": w_down}


def row_terms(token_rows, cot_rows, gate_w, up_w, down_w):
    gate_pre = jnp.dot(token_rows, gate_w.T, preferred_element_type=jnp.float32)
    up_pre = jnp.dot(token_rows, up_w.T, preferred_element_type=jnp.float32)
    sigmoid_gate = jax.nn.sigmoid(gate_pre)
    activation = gate_pre * sigmoid_gate
    hidden = (activation * up_pre).astype(jnp.bfloat16)
    hidden_grad = jnp.dot(cot_rows, down_w.T, preferred_element_type=jnp.float32)
    up_grad = (hidden_grad * activation).astype(jnp.bfloat16)
    gate_grad = (hidden_grad * up_pre * sigmoid_gate * (1.0 + gate_pre * (1.0 - sigmoid_gate))).astype(jnp.bfloat16)
    return hidden, gate_grad, up_grad


def expert_grads(operands):
    token_rows, cot_rows, gate_w, up_w, down_w = operands
    hidden, gate_grad, up_grad = row_terms(token_rows, cot_rows, gate_w, up_w, down_w)
    gate_out = jnp.dot(gate_grad.T, token_rows, preferred_element_type=jnp.float32).astype(jnp.bfloat16)
    up_out = jnp.dot(up_grad.T, token_rows, preferred_element_type=jnp.float32).astype(jnp.bfloat16)
    down_out = jnp.dot(hidden.T, cot_rows, preferred_element_type=jnp.float32).astype(jnp.bfloat16)
    return gate_out, up_out, down_out


def reference(tokens, cotangent, experts, slots, gates, w_gate, w_up, w_down):
    batches = TOKENS // TOK_F
    batch_index = (jnp.arange(TOKENS) // TOK_F).astype(jnp.int32)
    row_index = (batch_index[:, None] * CAP + slots).astype(jnp.int32)
    scaled = (gates[:, :, None] * cotangent[:, None, :].astype(jnp.float32)).astype(jnp.bfloat16)
    spread = jnp.broadcast_to(tokens[:, None, :], (TOKENS, TOPK, D))
    token_buffer = jnp.zeros((EXPERTS, batches * CAP, D), jnp.bfloat16).at[experts, row_index].set(spread)
    cot_buffer = jnp.zeros((EXPERTS, batches * CAP, D), jnp.bfloat16).at[experts, row_index].set(scaled)
    grads = lax.map(expert_grads, (token_buffer, cot_buffer, w_gate, w_up, w_down))
    return grads[0], grads[1], grads[2]
```

```python
import functools

import jax
import jax.numpy as jnp
from jax import lax
from jax.experimental import pallas as pl
from jax.experimental.pallas import tpu as pltpu
from jax.sharding import PartitionSpec as P


NT = (((1,), (1,)), ((), ()))
NN = (((1,), (0,)), ((), ()))


def dot(left, right, dims):
    return lax.dot_general(left, right, dims, preferred_element_type=jnp.float32)


def pick_kernel(experts, capacity, me_ref, experts_ref, slots_ref, gates_ref, tok_ref, cot_ref, *outs):
    codes = (experts_ref[...] ^ me_ref[0]) * capacity + slots_ref[...]
    tokens = codes.shape[1]
    rows = lax.broadcasted_iota(jnp.int32, (experts * capacity, tokens), 0)
    picker = jnp.zeros((experts * capacity, tokens), jnp.float32)
    weight = jnp.zeros((experts * capacity, tokens), jnp.float32)
    for k in range(codes.shape[0]):
        hit = rows == codes[k : k + 1, :]
        picker = picker + jnp.where(hit, 1.0, 0.0)
        weight = weight + jnp.where(hit, gates_ref[k : k + 1, :], 0.0)
    slot_gate = jnp.sum(weight, axis=1, keepdims=True)
    picker = picker.astype(jnp.bfloat16)
    tok = dot(picker, tok_ref[...], NN).astype(jnp.bfloat16)
    cot = (dot(picker, cot_ref[...], NN) * slot_gate).astype(jnp.bfloat16)
    for k in range(experts):
        outs[k][...] = tok[k * capacity : (k + 1) * capacity]
        outs[experts + k][...] = cot[k * capacity : (k + 1) * capacity]


def pick(me, experts, slots, gates, tokens, cotangent, count, capacity):
    feature = tokens.shape[1]
    vmem = pl.BlockSpec(memory_space=pltpu.VMEM)
    outs = pl.pallas_call(
        functools.partial(pick_kernel, count, capacity),
        in_specs=[pl.BlockSpec(memory_space=pltpu.SMEM)] + [vmem] * 5,
        out_specs=[vmem] * (2 * count),
        out_shape=[jax.ShapeDtypeStruct((capacity, feature), jnp.bfloat16)] * (2 * count),
        name="pick",
    )(me, experts.T, slots.T, gates.T, tokens, cotangent)
    return list(outs[:count]), list(outs[count:])


def swap(x, axis, bit):
    size = lax.axis_size(axis)
    return lax.ppermute(x, axis, [(i, i ^ bit) for i in range(size)])


def fold(have, bit):
    keys = list(have)
    cap = have[keys[0]].shape[0]
    sent = have[keys[0]] if len(keys) == 1 else jnp.concatenate([have[k] for k in keys], axis=0)
    got = swap(sent, "fsdp", bit)
    more = dict(have)
    for i, k in enumerate(keys):
        more[k ^ bit] = got[i * cap : (i + 1) * cap]
    return more


def to_experts(blocks):
    return [blocks[0]] + [swap(b, "expert", k) for k, b in enumerate(blocks) if k]


def halves(parts):
    half = len(parts) // 2
    return [{0: jnp.concatenate(parts[:half], axis=1)}, {0: jnp.concatenate(parts[half:], axis=1)}]


def after(values, others):
    return lax.optimization_barrier((values, others))[0]


def last_fold(have, bit):
    own = jnp.concatenate([have[k] for k in sorted(have)], axis=0)
    return [own, swap(own, "fsdp", bit)]


def gate_kernel(steps, me_ref, a0, a1, b0, b1, w_ref, out_ref):
    k = pl.program_id(0)
    part = dot(w_ref[0], stacked(k < steps // 2, a0, a1, b0, b1), NT)

    @pl.when(k == 0)
    def _():
        out_ref[...] = part

    @pl.when(k > 0)
    def _():
        out_ref[...] += part


def stacked(early, a0, a1, b0, b1):
    return jnp.concatenate(
        [jnp.where(early, a0[...], b0[...]), jnp.where(early, a1[...], b1[...])], axis=0
    )


def up_kernel(steps, me_ref, a0, a1, b0, b1, w_ref, gate_ref, hid_ref, act_ref, slope_ref, acc):
    k = pl.program_id(0)
    part = dot(w_ref[0], stacked(k < steps // 2, a0, a1, b0, b1), NT)

    @pl.when(k == 0)
    def _():
        acc[...] = part

    @pl.when(k > 0)
    def _():
        acc[...] += part

    @pl.when(k == steps - 1)
    def _():
        g = gate_ref[...]
        u = acc[...]
        s = jax.nn.sigmoid(g)
        act = g * s
        hid_ref[...] = (act * u).astype(jnp.bfloat16)
        act_ref[...] = act
        slope_ref[...] = u * s * (1.0 + g * (1.0 - s))


def piece_specs(array_rows, width, half, block_of):
    early = pl.BlockSpec((array_rows, width), lambda s, me: (0, jnp.clip(block_of(s), 0, half - 1)))
    late = pl.BlockSpec((array_rows, width), lambda s, me: (0, jnp.clip(block_of(s) - half, 0, half - 1)))
    return [early, early, late, late]


def forward(me, tok, weight, count, gate=None):
    rows = 2 * tok[0].shape[0]
    units, width = weight.shape[1:]
    feature = width // count
    whole = pl.BlockSpec((units, rows), lambda k, me: (0, 0))
    in_specs = piece_specs(rows // 2, feature, count // 2, lambda k: k) + [
        pl.BlockSpec((1, units, feature), lambda k, me: (0, 0, me[0] ^ k))
    ]
    f32 = jax.ShapeDtypeStruct((units, rows), jnp.float32)
    if gate is None:
        body, out_specs, out_shape, scratch, extra = gate_kernel, whole, f32, [], ()
    else:
        body = up_kernel
        in_specs = in_specs + [whole]
        out_specs = [whole] * 3
        out_shape = [jax.ShapeDtypeStruct((units, rows), jnp.bfloat16), f32, f32]
        scratch = [pltpu.VMEM((units, rows), jnp.float32)]
        extra = (gate,)
    return pl.pallas_call(
        functools.partial(body, count),
        grid_spec=pltpu.PrefetchScalarGridSpec(
            num_scalar_prefetch=1,
            grid=(count,),
            in_specs=in_specs,
            out_specs=out_specs,
            scratch_shapes=scratch,
        ),
        out_shape=out_shape,
        compiler_params=pltpu.CompilerParams(dimension_semantics=("arbitrary",)),
        cost_estimate=pl.CostEstimate(
            flops=2 * rows * units * width, bytes_accessed=2 * units * width, transcendentals=0
        ),
        name="gate" if gate is None else "up",
    )(me, *tok, weight, *extra)


def backward_kernel(steps, me_ref, *refs):
    cot_in, wd_ref, tok_in = refs[:4], refs[4], refs[5:9]
    hid_ref, act_ref, slope_ref, gg_ref, gu_ref, gd_ref, acc, gate_grad, up_grad = refs[9:]
    s = pl.program_id(0)

    @pl.when(s < steps)
    def _():
        part = dot(wd_ref[0], stacked(s < steps // 2, *cot_in), NT)

        @pl.when(s == 0)
        def _():
            acc[...] = part

        @pl.when(s > 0)
        def _():
            acc[...] += part

        @pl.when(s == steps - 1)
        def _():
            h = acc[...]
            up_grad[...] = (h * act_ref[...]).astype(jnp.bfloat16)
            gate_grad[...] = (h * slope_ref[...]).astype(jnp.bfloat16)

    @pl.when(s >= steps)
    def _():
        early = s < steps + steps // 2
        tok = stacked(early, *tok_in)
        cot = stacked(early, *cot_in)
        gg_ref[0] = dot(gate_grad[...], tok, NN).astype(jnp.bfloat16)
        gu_ref[0] = dot(up_grad[...], tok, NN).astype(jnp.bfloat16)
        gd_ref[0] = dot(hid_ref[...], cot, NN).astype(jnp.bfloat16)


def backward(me, tok, cot, hid, act, slope, w_down, count):
    rows = 2 * tok[0].shape[0]
    units, width = w_down.shape[1:]
    feature = width // count
    last = count - 1

    def late(s):
        return jnp.maximum(s - count, 0)

    whole = pl.BlockSpec((units, rows), lambda s, me: (0, 0))
    out_spec = pl.BlockSpec(
        (1, units, feature), lambda s, me: (0, 0, me[0] ^ late(s))
    )
    out = jax.ShapeDtypeStruct((1, units, width), jnp.bfloat16)
    return pl.pallas_call(
        functools.partial(backward_kernel, count),
        grid_spec=pltpu.PrefetchScalarGridSpec(
            num_scalar_prefetch=1,
            grid=(2 * count,),
            in_specs=piece_specs(rows // 2, feature, count // 2, lambda s: s % count)
            + [pl.BlockSpec((1, units, feature), lambda s, me: (0, 0, me[0] ^ jnp.minimum(s, last)))]
            + piece_specs(rows // 2, feature, count // 2, late)
            + [whole] * 3,
            out_specs=[out_spec, out_spec, out_spec],
            scratch_shapes=[
                pltpu.VMEM((units, rows), jnp.float32),
                pltpu.VMEM((units, rows), jnp.bfloat16),
                pltpu.VMEM((units, rows), jnp.bfloat16),
            ],
        ),
        out_shape=[out, out, out],
        compiler_params=pltpu.CompilerParams(dimension_semantics=("arbitrary",)),
        cost_estimate=pl.CostEstimate(
            flops=8 * rows * units * width, bytes_accessed=8 * units * width, transcendentals=0
        ),
        name="backward",
    )(me, *cot, w_down, *tok, hid, act, slope)


def local(tokens, cotangent, experts, slots, gates, w_gate, w_up, w_down):
    count = lax.axis_size("expert")
    per_expert = tokens.shape[0] // count
    capacity = min(5 * per_expert // 2, per_expert * count)
    me = lax.axis_index("expert").astype(jnp.int32).reshape(1)
    tok_blocks, cot_blocks = pick(me, experts, slots, gates, tokens, cotangent, count, capacity)
    bits = []
    bit = 1
    while bit < lax.axis_size("fsdp"):
        bits.append(bit)
        bit *= 2
    orders = list(zip(bits[1:], bits[:0:-1]))
    tok_parts = to_experts(tok_blocks)
    tok = halves(tok_parts)
    cot = halves(to_experts(after(cot_blocks, tok_parts)))
    for pair in orders:
        tok = [fold(have, b) for have, b in zip(tok, pair)]
    tok, cot = lax.optimization_barrier((tok, cot))
    tok = last_fold(tok[0], bits[0]) + last_fold(tok[1], bits[0])
    cot = [fold(have, b) for have, b in zip(cot, orders[0])]
    gate = forward(me, tok, w_gate, count)
    cot, gate = lax.optimization_barrier((cot, gate))
    for pair in orders[1:]:
        cot = [fold(have, b) for have, b in zip(cot, pair)]
    hid, act, slope = forward(me, tok, w_up, count, gate)
    cot = after(cot, hid)
    cot = last_fold(cot[0], bits[0]) + last_fold(cot[1], bits[0])
    return tuple(backward(me, tok, cot, hid, act, slope, w_down, count))


def solution(mesh):
    return jax.shard_map(
        local,
        mesh=mesh,
        in_specs=(
            P("fsdp", "expert"),
            P("fsdp", "expert"),
            P("fsdp", None),
            P("fsdp", None),
            P("fsdp", None),
            P("expert", "fsdp", None),
            P("expert", "fsdp", None),
            P("expert", "fsdp", None),
        ),
        out_specs=(P("expert", "fsdp", None), P("expert", "fsdp", None), P("expert", "fsdp", None)),
        check_vma=False,
    )
```
